8 devices in a mesh: dp: 1 (over z), tp: 8 (over y, x, core).
Axes of the slice: x: 2, y: 2, z: 1, core: 2. Of those that a mesh axis runs over, the one named last changes fastest.
Arguments:
- x: bfloat16 [24, 384, 5120], P('dp')
- seq_lens: int32 [24], P('dp')
- w_query: bfloat16 [5120, 5120], P(None, 'tp')
- w_key: bfloat16 [5120, 1024], P(None, 'tp')
- w_value: bfloat16 [5120, 1024], P(None, 'tp')
- w_out: bfloat16 [5120, 5120], P('tp')
- w_gate: bfloat16 [5120, 27648], P(None, 'tp')
- w_up: bfloat16 [5120, 27648], P(None, 'tp')
- w_down: bfloat16 [27648, 5120], P('tp')
- attn_gain: bfloat16 [5120], replicated
- mlp_gain: bfloat16 [5120], replicated
- k_cache: bfloat16 [24, 768, 8, 128], P('dp', None, 'tp')
- v_cache: bfloat16 [24, 768, 8, 128], P('dp', None, 'tp')
Outputs:
- output 1: bfloat16 [24, 384, 5120], P('dp')
- output 2: bfloat16 [24, 768, 8, 128], P('dp', None, 'tp')
- output 3: bfloat16 [24, 768, 8, 128], P('dp', None, 'tp')
All inputs are finite; a program needn't handle non-finite values.
Results may differ from the reference program's by a relative error of at most 0.0114497.
Values are sent between devices in bfloat16 or wider.
A program may use at most 1.25 GiB of HBM per device.

```python
import jax
import jax.numpy as jnp
from jax import lax

D = 5120
HEADS = 40
KV_HEADS = 8
HEAD = 128
FF = 27648
BATCH = 24
SEQ = 384
CACHE_LEN = 768
TP = 8
EPS = 1e-5
ROPE_BASE = 10000.0


def setup_inputs(seed: int = 0, part: int = 0) -> dict:
    base_key = jax.random.key(seed)
    part_key = jax.random.fold_in(base_key, part)
    weight_keys = jax.random.split(base_key, 9)
    part_keys = jax.random.split(part_key, 5)
    qk_scale = 1.5 * D ** -0.5

    def normal_weight(rng_key, array_shape, factor):
        return (jax.random.normal(rng_key, array_shape, jnp.float32) * factor).astype(jnp.bfloat16)

    short_len = jax.random.randint(part_keys[1], (1,), SEQ // 2, (4 * SEQ) // 5 + 1)
    other_lens = jax.random.randint(part_keys[2], (BATCH - 1,), SEQ // 2, SEQ + 1)
    return {
        "x": normal_weight(part_keys[0], (BATCH, SEQ, D), 1.0),
        "seq_lens": jnp.concatenate([short_len, other_lens]).astype(jnp.int32),
        "w_query": normal_weight(weight_keys[0], (D, HEADS * HEAD), qk_scale),
        "w_key": normal_weight(weight_keys[1], (D, KV_HEADS * HEAD), qk_scale),
        "w_value": normal_weight(weight_keys[2], (D, KV_HEADS * HEAD), D ** -0.5),
        "w_out": normal_weight(weight_keys[3], (HEADS * HEAD, D), (HEADS * HEAD) ** -0.5),
        "w_gate": normal_weight(weight_keys[4], (D, FF), D ** -0.5),
        "w_up": normal_weight(weight_keys[5], (D, FF), D ** -0.5),
        "w_down": normal_weight(weight_keys[6], (FF, D), FF ** -0.5),
        "attn_gain": jax.random.uniform(weight_keys[7], (D,), jnp.float32, 0.5, 1.5).astype(jnp.bfloat16),
        "mlp_gain": jax.random.uniform(weight_keys[8], (D,), jnp.float32, 0.5, 1.5).astype(jnp.bfloat16),
        "k_cache": normal_weight(part_keys[3], (BATCH, CACHE_LEN, KV_HEADS, HEAD), 1.0),
        "v_cache": normal_weight(part_keys[4], (BATCH, CACHE_LEN, KV_HEADS, HEAD), 1.0),
    }


def rms_norm(rows, gain):
    rows32 = rows.astype(jnp.float32)
    inv_rms = lax.rsqrt(jnp.mean(rows32 * rows32, axis=-1, keepdims=True) + EPS)
    return (rows32 * inv_rms * gain.astype(jnp.float32)).astype(jnp.bfloat16)


def rotary(vecs, angles):
    half_dim = HEAD // 2
    pairs = vecs.reshape(vecs.shape[:-1] + (half_dim, 2))
    even_part = pairs[..., 0]
    odd_part = pairs[..., 1]
    cos_tab = jnp.cos(angles)[:, None, :]
    sin_tab = jnp.sin(angles)[:, None, :]
    turned = jnp.stack([even_part * cos_tab - odd_part * sin_tab, even_part * sin_tab + odd_part * cos_tab], axis=-1)
    return turned.reshape(vecs.shape)


def reference(x, seq_lens, w_query, w_key, w_value, w_out, w_gate, w_up, w_down, attn_gain, mlp_gain, k_cache, v_cache):
    group_size = HEADS // KV_HEADS
    heads_part = HEADS * HEAD // TP
    ff_part = FF // TP
    positions = jnp.arange(SEQ)
    inv_freq = ROPE_BASE ** (-jnp.arange(0, HEAD, 2).astype(jnp.float32) / HEAD)
    angles = positions.astype(jnp.float32)[:, None] * inv_freq[None, :]
    causal = positions[None, :] <= positions[:, None]

    def one_sequence(items):
        x_row, length = items
        normed = rms_norm(x_row, attn_gain)
        queries = rotary(jnp.dot(normed, w_query, preferred_element_type=jnp.float32).reshape(SEQ, HEADS, HEAD), angles).astype(jnp.bfloat16)
        keys = rotary(jnp.dot(normed, w_key, preferred_element_type=jnp.float32).reshape(SEQ, KV_HEADS, HEAD), angles).astype(jnp.bfloat16)
        values = jnp.dot(normed, w_value, preferred_element_type=jnp.float32).astype(jnp.bfloat16).reshape(SEQ, KV_HEADS, HEAD)
        valid = positions < length
        keys = jnp.where(valid[:, None, None], keys, jnp.zeros_like(keys))
        values = jnp.where(valid[:, None, None], values, jnp.zeros_like(values))
        allowed = causal & valid[None, :]

        def one_kv_head(blocks):
            q_block, k_block, v_block = blocks
            scores = jnp.einsum("qgh,sh->gqs", q_block.astype(jnp.float32), k_block.astype(jnp.float32)) * HEAD ** -0.5
            scores = jnp.where(allowed[None], scores, -jnp.inf)
            probs = jax.nn.softmax(scores, axis=-1).astype(jnp.bfloat16)
            mixed = jnp.einsum("gqs,sh->qgh", probs.astype(jnp.float32), v_block.astype(jnp.float32))
            return mixed.astype(jnp.bfloat16)

        q_grouped = jnp.transpose(queries.reshape(SEQ, KV_HEADS, group_size, HEAD), (1, 0, 2, 3))
        head_out = lax.map(one_kv_head, (q_grouped, jnp.transpose(keys, (1, 0, 2)), jnp.transpose(values, (1, 0, 2))))
        attn_rows = jnp.transpose(head_out, (1, 0, 2, 3)).reshape(SEQ, HEADS * HEAD)
        attn_sum = jnp.zeros((SEQ, D), jnp.float32)
        for index in range(TP):
            partial = jnp.dot(attn_rows[:, index * heads_part:(index + 1) * heads_part], w_out[index * heads_part:(index + 1) * heads_part], preferred_element_type=jnp.float32)
            attn_sum = attn_sum + partial.astype(jnp.bfloat16).astype(jnp.float32)
        hidden = (x_row.astype(jnp.float32) + attn_sum).astype(jnp.bfloat16)
        normed_mlp = rms_norm(hidden, mlp_gain)
        gate_pre = jnp.dot(normed_mlp, w_gate, preferred_element_type=jnp.float32)
        up_pre = jnp.dot(normed_mlp, w_up, preferred_element_type=jnp.float32)
        gated = (jax.nn.silu(gate_pre) * up_pre).astype(jnp.bfloat16)
        mlp_sum = jnp.zeros((SEQ, D), jnp.float32)
        for index in range(TP):
            partial = jnp.dot(gated[:, index * ff_part:(index + 1) * ff_part], w_down[index * ff_part:(index + 1) * ff_part], preferred_element_type=jnp.float32)
            mlp_sum = mlp_sum + partial.astype(jnp.bfloat16).astype(jnp.float32)
        out_row = (hidden.astype(jnp.float32) + mlp_sum).astype(jnp.bfloat16)
        return out_row, keys, values

    y, new_keys, new_values = lax.map(one_sequence, (x, seq_lens))
    k_cache_out = lax.dynamic_update_slice(k_cache, new_keys, (0, 0, 0, 0))
    v_cache_out = lax.dynamic_update_slice(v_cache, new_values, (0, 0, 0, 0))
    return y, k_cache_out, v_cache_out
```

```python
import functools

import jax
import jax.numpy as jnp
from jax import lax
from jax.experimental import pallas as pl
from jax.experimental.pallas import tpu as pltpu
from jax.sharding import PartitionSpec as P


EPS = 1e-5
ROPE_BASE = 10000.0
CHUNKS = (6, 6, 6, 4, 2)
SETTLED = 2
Q_BLOCK = 128
COL_TILE = 512


def norm_rows(src_ref, dst_ref, gain_ref, rows, step):
    gain = gain_ref[...].astype(jnp.float32)

    def body(index, carry):
        part = pl.ds(pl.multiple_of(index * step, step), step)
        rows32 = src_ref[part, :].astype(jnp.float32)
        inv_rms = lax.rsqrt(jnp.mean(rows32 * rows32, axis=-1, keepdims=True) + EPS)
        dst_ref[part, :] = (rows32 * inv_rms * gain).astype(jnp.bfloat16)
        return carry

    lax.fori_loop(0, rows // step, body, 0)


def attend_kernel(first, lens_ref, x_ref, wq_ref, wkv_ref, gain_ref, cos_ref, sin_ref, o_ref, k_ref, v_ref, normed_ref):
    seq_len = x_ref.shape[0]
    head_dim = cos_ref.shape[1]
    group_size = wq_ref.shape[1] // head_dim
    length = lens_ref[first + pl.program_id(0)]
    norm_rows(x_ref, normed_ref, gain_ref, seq_len, 16)
    normed = normed_ref[...]
    kv_pre = jnp.dot(normed, wkv_ref[...], preferred_element_type=jnp.float32)
    q_pre = jnp.dot(normed, wq_ref[...], preferred_element_type=jnp.float32)
    cos_tab = cos_ref[...]
    sin_tab = sin_ref[...]
    even_lane = lax.broadcasted_iota(jnp.int32, (seq_len, head_dim), 1) % 2 == 0

    def rotate(vecs):
        swapped = jnp.where(even_lane, pltpu.roll(vecs, head_dim - 1, 1), pltpu.roll(vecs, 1, 1))
        return (vecs * cos_tab + swapped * sin_tab).astype(jnp.bfloat16)

    valid = lax.broadcasted_iota(jnp.int32, (seq_len, head_dim), 0) < length
    keys32 = jnp.where(valid, rotate(kv_pre[:, :head_dim]).astype(jnp.float32), 0.0)
    values32 = jnp.where(valid, kv_pre[:, head_dim:], 0.0)
    keys = keys32.astype(jnp.bfloat16)
    values = values32.astype(jnp.bfloat16)
    k_ref[...] = keys
    v_ref[...] = values
    queries = [rotate(q_pre[:, j * head_dim:(j + 1) * head_dim]) for j in range(group_size)]
    for block in range(seq_len // Q_BLOCK):
        lo, hi = block * Q_BLOCK, (block + 1) * Q_BLOCK
        t_pos = lo + lax.broadcasted_iota(jnp.int32, (Q_BLOCK, hi), 0)
        u_pos = lax.broadcasted_iota(jnp.int32, (Q_BLOCK, hi), 1)
        allowed = (u_pos <= t_pos) & (u_pos < length)
        for j in range(group_size):
            scores = lax.dot_general(queries[j][lo:hi], keys[:hi], (((1,), (1,)), ((), ())), preferred_element_type=jnp.float32) * head_dim ** -0.5
            scores = jnp.where(allowed, scores, -jnp.inf)
            expd = jnp.exp(scores - jnp.max(scores, axis=-1, keepdims=True))
            probs = (expd / jnp.sum(expd, axis=-1, keepdims=True)).astype(jnp.bfloat16)
            o_ref[lo:hi, j * head_dim:(j + 1) * head_dim] = jnp.dot(probs, values[:hi], preferred_element_type=jnp.float32).astype(jnp.bfloat16)


def attend(first, count, x, seq_lens, w_query, w_kv, gain, cos_tab, sin_tab):
    _, seq_len, width = x.shape
    q_cols = w_query.shape[1]
    head_dim = cos_tab.shape[1]
    whole = lambda *shape: pl.BlockSpec(shape, lambda b, lens: (0,) * len(shape))
    per_seq = lambda cols: pl.BlockSpec((None, seq_len, cols), lambda b, lens: (b, 0, 0))
    grid_spec = pltpu.PrefetchScalarGridSpec(
        num_scalar_prefetch=1,
        grid=(count,),
        in_specs=[
            pl.BlockSpec((None, seq_len, width), lambda b, lens: (first + b, 0, 0)),
            whole(width, q_cols),
            whole(width, 2 * head_dim),
            whole(1, width),
            whole(seq_len, head_dim),
            whole(seq_len, head_dim),
        ],
        out_specs=[per_seq(q_cols), per_seq(head_dim), per_seq(head_dim)],
        scratch_shapes=[pltpu.VMEM((seq_len, width), jnp.bfloat16)],
    )
    return pl.pallas_call(
        functools.partial(attend_kernel, first),
        grid_spec=grid_spec,
        out_shape=[jax.ShapeDtypeStruct((count, seq_len, cols), jnp.bfloat16) for cols in (q_cols, head_dim, head_dim)],
        compiler_params=pltpu.CompilerParams(vmem_limit_bytes=56 * 1024 * 1024),
        cost_estimate=pl.CostEstimate(flops=2 * count * seq_len * width * (q_cols + 2 * head_dim), bytes_accessed=2 * count * seq_len * (width + q_cols), transcendentals=0),
        name="attend",
    )(seq_lens, x, w_query, w_kv, gain, cos_tab, sin_tab)


def project_kernel(o_ref, w_ref, x_ref, gain_ref, h_ref, n_ref):
    groups, rows, depth = o_ref.shape
    tile = w_ref.shape[1]
    columns = pl.ds(pl.multiple_of(pl.program_id(0) * tile, tile), tile)
    total = jnp.zeros((rows, tile), jnp.float32)
    for index in range(groups):
        partial = jnp.dot(o_ref[index], w_ref[index * depth:(index + 1) * depth, :], preferred_element_type=jnp.float32)
        total = total + partial.astype(jnp.bfloat16).astype(jnp.float32)
    h_ref[:, columns] = (x_ref[...].astype(jnp.float32) + total).astype(jnp.bfloat16)

    @pl.when(pl.program_id(0) == pl.num_programs(0) - 1)
    def _():
        norm_rows(h_ref, n_ref, gain_ref, rows, 16)


def project(o_all, w_out_all, x_rows, gain):
    groups, rows, depth = o_all.shape
    width = w_out_all.shape[1]
    out = jax.ShapeDtypeStruct((rows, width), jnp.bfloat16)
    return pl.pallas_call(
        project_kernel,
        grid=(width // COL_TILE,),
        in_specs=[
            pl.BlockSpec((groups, rows, depth), lambda j: (0, 0, 0)),
            pl.BlockSpec((groups * depth, COL_TILE), lambda j: (0, j)),
            pl.BlockSpec((rows, COL_TILE), lambda j: (0, j)),
            pl.BlockSpec((1, width), lambda j: (0, 0)),
        ],
        out_specs=[pl.BlockSpec((rows, width), lambda j: (0, 0))] * 2,
        out_shape=[out, out],
        compiler_params=pltpu.CompilerParams(vmem_limit_bytes=48 * 1024 * 1024),
        cost_estimate=pl.CostEstimate(flops=2 * rows * groups * depth * width, bytes_accessed=2 * (groups * depth * width + 4 * rows * width), transcendentals=0),
        name="project",
    )(o_all, w_out_all, x_rows, gain)


def solution(mesh):
    tp_size = mesh.shape["tp"]
    last = len(CHUNKS) - 1

    def swap(value, bit):
        return lax.ppermute(value, "tp", [(index, index ^ bit) for index in range(tp_size)])

    def sum_partials(partial, resid_rows):
        rows, width = resid_rows.shape
        half = rows // 2
        me = lax.axis_index("tp")
        core, chip = me % 2, me // 2
        blocks = partial.reshape(tp_size // 2, 2, rows, width)
        take = lambda which: lax.dynamic_index_in_dim(blocks, which, 1, keepdims=False)
        ours = take(core)
        theirs = swap(take(1 - core), 1)

        def both(step, lo):
            pick = lambda value: lax.dynamic_slice(value, (chip ^ step, lo, 0), (1, half, width))[0].astype(jnp.float32)
            return pick(ours) + pick(theirs)

        x_far, y_far = swap(both(3, 0), 2), swap(both(3, half), 4)
        x_near, y_near = swap(both(1, 0), 2), swap(both(2, half), 4)
        x_late = swap(both(1, half) + y_far, 2)
        y_late = swap(both(2, 0) + x_far, 4)
        upper = resid_rows[:half].astype(jnp.float32) + (both(0, 0) + x_near + y_late)
        lower = resid_rows[half:].astype(jnp.float32) + (both(0, half) + x_late + y_near)
        return jnp.concatenate([upper.astype(jnp.bfloat16), lower.astype(jnp.bfloat16)], axis=0)

    def layer_shard(x, seq_lens, w_query, w_key, w_value, w_out, w_gate, w_up, w_down, attn_gain, mlp_gain, k_cache, v_cache):
        batch_size, seq_len, width = x.shape
        head_dim = k_cache.shape[3]
        tp_index = lax.axis_index("tp")
        w_out_all = lax.all_gather(w_out, "tp", axis=0, tiled=True)
        w_kv = jnp.concatenate([w_key, w_value], axis=1)
        inv_freq = ROPE_BASE ** (-jnp.arange(0, head_dim, 2).astype(jnp.float32) / head_dim)
        angles = jnp.repeat(jnp.arange(seq_len).astype(jnp.float32)[:, None] * inv_freq[None, :], 2, axis=1)
        sign = jnp.where(jnp.arange(head_dim) % 2 == 0, -1.0, 1.0)
        cos_tab = jnp.cos(angles)
        sin_tab = jnp.sin(angles) * sign
        x_flat = x.reshape(batch_size * seq_len, width)
        y = jnp.zeros((batch_size * seq_len, width), jnp.bfloat16)
        gathered = []
        starts = [sum(CHUNKS[:index]) for index in range(len(CHUNKS))]
        attended, received = [], []
        for first, count in zip(starts, CHUNKS):
            attended.append(attend(first, count, x, seq_lens, w_query, w_kv, attn_gain[None], cos_tab, sin_tab))
            received.append(lax.all_to_all(attended[-1][0].reshape(tp_size, count * seq_len // tp_size, -1), "tp", 0, 0, tiled=True))
        new_keys = [keys for _, keys, _ in attended]
        new_values = [values for _, _, values in attended]
        w_out_all, new_keys = lax.optimization_barrier((w_out_all, new_keys))
        for index, (first, count) in enumerate(zip(starts, CHUNKS)):
            start_row = first * seq_len
            rows = count * seq_len // tp_size
            x_rows = lax.dynamic_slice_in_dim(x_flat, start_row + tp_index * rows, rows, axis=0)
            hidden, normed = project(received[index], w_out_all, x_rows, mlp_gain[None])
            normed_all = lax.all_gather(normed, "tp", axis=0, tiled=True)
            gate_pre = jnp.dot(normed_all, w_gate, preferred_element_type=jnp.float32)
            up_pre = jnp.dot(normed_all, w_up, preferred_element_type=jnp.float32)
            gated = (jax.nn.silu(gate_pre) * up_pre).astype(jnp.bfloat16)
            if index == last:
                gated, settled = lax.optimization_barrier((gated, gathered[:SETTLED]))
                for row, block in zip(starts, settled):
                    y = lax.dynamic_update_slice(y, block, (row * seq_len, 0))
                gated, y = lax.optimization_barrier((gated, y))
            mlp_part = jnp.dot(gated, w_down, preferred_element_type=jnp.float32).astype(jnp.bfloat16)
            out_rows = sum_partials(mlp_part, hidden)
            gathered.append(lax.all_gather(out_rows, "tp", axis=0, tiled=True))
        for index in range(SETTLED, len(CHUNKS)):
            y = lax.dynamic_update_slice(y, gathered[index], (starts[index] * seq_len, 0))
        k_cache_out = lax.dynamic_update_slice(k_cache, jnp.concatenate(new_keys)[:, :, None, :], (0, 0, 0, 0))
        v_cache_out = lax.dynamic_update_slice(v_cache, jnp.concatenate(new_values)[:, :, None, :], (0, 0, 0, 0))
        return y.reshape(x.shape), k_cache_out, v_cache_out

    cache_spec = P("dp", None, "tp", None)
    return jax.shard_map(layer_shard, mesh=mesh, in_specs=(P("dp", None, None), P("dp"), P(None, "tp"), P(None, "tp"), P(None, "tp"), P("tp", None), P(None, "tp"), P(None, "tp"), P("tp", None), P(), P(), cache_spec, cache_spec), out_specs=(P("dp", None, None), cache_spec, cache_spec), check_vma=False)
```

```python
import functools

import jax
import jax.numpy as jnp
from jax import lax
from jax.experimental import pallas as pl
from jax.experimental.pallas import tpu as pltpu
from jax.sharding import PartitionSpec as P


EPS = 1e-5
ROPE_BASE = 10000.0
CHUNKS = (6, 6, 5, 4, 3)
PLACE_ROWS = 128
Q_BLOCK = 128
COL_TILE = 512


def norm_rows(src_ref, dst_ref, gain_ref, rows):
    def body(index, carry):
        parts = [pl.ds(pl.multiple_of(index * 48 + shift, 16), 16) for shift in (0, 16, 32)]
        inv_rms = []
        for part in parts:
            rows32 = src_ref[part, :].astype(jnp.float32)
            inv_rms.append(lax.rsqrt(jnp.mean(rows32 * rows32, axis=-1, keepdims=True) + EPS))
        for part, inv in zip(parts, inv_rms):
            dst_ref[part, :] = (src_ref[part, :].astype(jnp.float32) * inv * gain_ref[...].astype(jnp.float32)).astype(jnp.bfloat16)
        return carry

    lax.fori_loop(0, rows // 48, body, 0)


def attend_kernel(first, lens_ref, x_ref, wq_ref, wkv_ref, gain_ref, cos_ref, sin_ref, o_ref, k_ref, v_ref, normed_ref):
    seq_len = x_ref.shape[0]
    head_dim = cos_ref.shape[1]
    group_size = wq_ref.shape[1] // head_dim
    length = lens_ref[first + pl.program_id(0)]
    norm_rows(x_ref, normed_ref, gain_ref, seq_len)
    normed = normed_ref[...]
    kv_pre = jnp.dot(normed, wkv_ref[...], preferred_element_type=jnp.float32)
    q_pre = jnp.dot(normed, wq_ref[...], preferred_element_type=jnp.float32)
    cos_tab = cos_ref[...]
    sin_tab = sin_ref[...]
    even_lane = lax.broadcasted_iota(jnp.int32, (seq_len, head_dim), 1) % 2 == 0

    def rotate(vecs):
        swapped = jnp.where(even_lane, pltpu.roll(vecs, head_dim - 1, 1), pltpu.roll(vecs, 1, 1))
        return (vecs * cos_tab + swapped * sin_tab).astype(jnp.bfloat16)

    valid = lax.broadcasted_iota(jnp.int32, (seq_len, head_dim), 0) < length
    keys32 = jnp.where(valid, rotate(kv_pre[:, :head_dim]).astype(jnp.float32), 0.0)
    values32 = jnp.where(valid, kv_pre[:, head_dim:], 0.0)
    keys = keys32.astype(jnp.bfloat16)
    values = values32.astype(jnp.bfloat16)
    k_ref[...] = keys
    v_ref[...] = values
    queries = [rotate(q_pre[:, j * head_dim:(j + 1) * head_dim]) for j in range(group_size)]
    for block in range(seq_len // Q_BLOCK):
        lo, hi = block * Q_BLOCK, (block + 1) * Q_BLOCK
        t_pos = lo + lax.broadcasted_iota(jnp.int32, (Q_BLOCK, hi), 0)
        u_pos = lax.broadcasted_iota(jnp.int32, (Q_BLOCK, hi), 1)
        allowed = (u_pos <= t_pos) & (u_pos < length)
        for j in range(group_size):
            scores = lax.dot_general(queries[j][lo:hi], keys[:hi], (((1,), (1,)), ((), ())), preferred_element_type=jnp.float32) * head_dim ** -0.5
            scores = jnp.where(allowed, scores, -jnp.inf)
            expd = jnp.exp(scores - jnp.max(scores, axis=-1, keepdims=True))
            probs = (expd * (1.0 / jnp.sum(expd, axis=-1, keepdims=True))).astype(jnp.bfloat16)
            o_ref[lo:hi, j * head_dim:(j + 1) * head_dim] = jnp.dot(probs, values[:hi], preferred_element_type=jnp.float32).astype(jnp.bfloat16)


def attend(first, count, x, seq_lens, w_query, w_kv, gain, cos_tab, sin_tab):
    _, seq_len, width = x.shape
    q_cols = w_query.shape[1]
    head_dim = cos_tab.shape[1]
    whole = lambda *shape: pl.BlockSpec(shape, lambda b, lens: (0,) * len(shape))
    per_seq = lambda cols: pl.BlockSpec((None, seq_len, cols), lambda b, lens: (b, 0, 0))
    grid_spec = pltpu.PrefetchScalarGridSpec(
        num_scalar_prefetch=1,
        grid=(count,),
        in_specs=[
            pl.BlockSpec((None, seq_len, width), lambda b, lens: (first + b, 0, 0)),
            whole(width, q_cols),
            whole(width, 2 * head_dim),
            whole(1, width),
            whole(seq_len, head_dim),
            whole(seq_len, head_dim),
        ],
        out_specs=[per_seq(q_cols), per_seq(head_dim), per_seq(head_dim)],
        scratch_shapes=[pltpu.VMEM((seq_len, width), jnp.bfloat16)],
    )
    return pl.pallas_call(
        functools.partial(attend_kernel, first),
        grid_spec=grid_spec,
        out_shape=[jax.ShapeDtypeStruct((count, seq_len, cols), jnp.bfloat16) for cols in (q_cols, head_dim, head_dim)],
        compiler_params=pltpu.CompilerParams(vmem_limit_bytes=56 * 1024 * 1024),
        cost_estimate=pl.CostEstimate(flops=2 * count * seq_len * width * (q_cols + 2 * head_dim), bytes_accessed=2 * count * seq_len * (width + q_cols), transcendentals=0),
        name="attend",
    )(seq_lens, x, w_query, w_kv, gain, cos_tab, sin_tab)


def project_kernel(o_ref, w_ref, x_ref, gain_ref, h_ref, n_ref):
    groups, rows, depth = o_ref.shape
    tile = w_ref.shape[1]
    columns = pl.ds(pl.multiple_of(pl.program_id(0) * tile, tile), tile)
    total = jnp.zeros((rows, tile), jnp.float32)
    for index in range(groups):
        partial = jnp.dot(o_ref[index], w_ref[index * depth:(index + 1) * depth, :], preferred_element_type=jnp.float32)
        total = total + partial.astype(jnp.bfloat16).astype(jnp.float32)
    h_ref[:, columns] = (x_ref[...].astype(jnp.float32) + total).astype(jnp.bfloat16)

    @pl.when(pl.program_id(0) == pl.num_programs(0) - 1)
    def _():
        norm_rows(h_ref, n_ref, gain_ref, rows)


def project(o_all, w_out_all, x_rows, gain):
    groups, rows, depth = o_all.shape
    width = w_out_all.shape[1]
    out = jax.ShapeDtypeStruct((rows, width), jnp.bfloat16)
    return pl.pallas_call(
        project_kernel,
        grid=(width // COL_TILE,),
        in_specs=[
            pl.BlockSpec((groups, rows, depth), lambda j: (0, 0, 0)),
            pl.BlockSpec((groups * depth, COL_TILE), lambda j: (0, j)),
            pl.BlockSpec((rows, COL_TILE), lambda j: (0, j)),
            pl.BlockSpec((1, width), lambda j: (0, 0)),
        ],
        out_specs=[pl.BlockSpec((rows, width), lambda j: (0, 0))] * 2,
        out_shape=[out, out],
        compiler_params=pltpu.CompilerParams(vmem_limit_bytes=48 * 1024 * 1024),
        cost_estimate=pl.CostEstimate(flops=2 * rows * groups * depth * width, bytes_accessed=2 * (groups * depth * width + 4 * rows * width), transcendentals=0),
        name="project",
    )(o_all, w_out_all, x_rows, gain)


def place_kernel(block_ref, *refs):
    refs[-1][...] = block_ref[...]


def place(y, block, start, total_rows):
    rows, width = block.shape
    operands = [block] if y is None else [block, y]
    return pl.pallas_call(
        place_kernel,
        grid=(rows // PLACE_ROWS,),
        in_specs=[pl.BlockSpec((PLACE_ROWS, width), lambda i: (i, 0)), pl.BlockSpec(memory_space=pl.ANY)][:len(operands)],
        out_specs=pl.BlockSpec((PLACE_ROWS, width), lambda i: (start // PLACE_ROWS + i, 0)),
        out_shape=jax.ShapeDtypeStruct((total_rows, width), jnp.bfloat16),
        input_output_aliases={} if y is None else {1: 0},
        compiler_params=pltpu.CompilerParams(vmem_limit_bytes=16 * 1024 * 1024),
        cost_estimate=pl.CostEstimate(flops=rows * width, bytes_accessed=4 * rows * width, transcendentals=0),
        name="place",
    )(*operands)


def solution(mesh):
    tp_size = mesh.shape["tp"]
    last = len(CHUNKS) - 1

    def swap(value, bit):
        return lax.ppermute(value, "tp", [(index, index ^ bit) for index in range(tp_size)])

    def sum_partials(partial, resid_rows):
        rows, width = resid_rows.shape
        half = rows // 2
        me = lax.axis_index("tp")
        core, chip = me % 2, me // 2
        theirs = swap(partial, 1)

        def both(step, lo):
            start = (2 * (chip ^ step) + core) * rows + lo
            pick = lambda value: lax.dynamic_slice(value, (start, 0), (half, width)).astype(jnp.float32)
            return pick(partial) + pick(theirs)

        x_far, y_far = swap(both(3, 0), 2), swap(both(3, half), 4)
        x_near, y_near = swap(both(1, 0), 2), swap(both(2, half), 4)
        x_late = swap(both(1, half) + y_far, 2)
        y_late = swap(both(2, 0) + x_far, 4)
        upper = resid_rows[:half].astype(jnp.float32) + (both(0, 0) + x_near + y_late)
        lower = resid_rows[half:].astype(jnp.float32) + (both(0, half) + x_late + y_near)
        return jnp.concatenate([upper.astype(jnp.bfloat16), lower.astype(jnp.bfloat16)], axis=0)

    def layer_shard(x, seq_lens, w_query, w_key, w_value, w_out, w_gate, w_up, w_down, attn_gain, mlp_gain, k_cache, v_cache):
        batch_size, seq_len, width = x.shape
        head_dim = k_cache.shape[3]
        tp_index = lax.axis_index("tp")
        w_out_all = lax.all_gather(w_out, "tp", axis=0, tiled=True)
        w_kv = jnp.concatenate([w_key, w_value], axis=1)
        inv_freq = ROPE_BASE ** (-jnp.arange(0, head_dim, 2).astype(jnp.float32) / head_dim)
        angles = jnp.repeat(jnp.arange(seq_len).astype(jnp.float32)[:, None] * inv_freq[None, :], 2, axis=1)
        sign = jnp.where(jnp.arange(head_dim) % 2 == 0, -1.0, 1.0)
        cos_tab = jnp.cos(angles)
        sin_tab = jnp.sin(angles) * sign
        x_flat = x.reshape(batch_size * seq_len, width)
        y = None
        gathered = []

        def settle(y, block, index):
            return place(y, block, sum(CHUNKS[:index]) * seq_len, batch_size * seq_len)

        starts = [sum(CHUNKS[:index]) for index in range(len(CHUNKS))]
        attended, received = [], []
        for first, count in zip(starts, CHUNKS):
            attended.append(attend(first, count, x, seq_lens, w_query, w_kv, attn_gain[None], cos_tab, sin_tab))
            received.append(lax.all_to_all(attended[-1][0].reshape(tp_size, count * seq_len // tp_size, -1), "tp", 0, 0, tiled=True))
        new_keys = [keys for _, keys, _ in attended]
        new_values = [values for _, _, values in attended]
        w_out_all, new_keys = lax.optimization_barrier((w_out_all, new_keys))
        for index, (first, count) in enumerate(zip(starts, CHUNKS)):
            start_row = first * seq_len
            rows = count * seq_len // tp_size
            x_rows = lax.dynamic_slice_in_dim(x_flat, start_row + tp_index * rows, rows, axis=0)
            hidden, normed = project(received[index], w_out_all, x_rows, mlp_gain[None])
            normed_all = lax.all_gather(normed, "tp", axis=0, tiled=True)
            gate_pre = jnp.dot(normed_all, w_gate, preferred_element_type=jnp.float32)
            up_pre = jnp.dot(normed_all, w_up, preferred_element_type=jnp.float32)
            gated = (jax.nn.silu(gate_pre) * up_pre).astype(jnp.bfloat16)
            mlp_part = jnp.dot(gated, w_down, preferred_element_type=jnp.float32).astype(jnp.bfloat16)
            if index >= 2:
                mlp_part, settled = lax.optimization_barrier((mlp_part, gathered[index - 2]))
                y = settle(y, settled, index - 2)
            out_rows = sum_partials(mlp_part, hidden)
            gathered.append(lax.all_gather(out_rows, "tp", axis=0, tiled=True))
        for index in (last - 1, last):
            y = settle(y, gathered[index], index)
        k_cache_out = lax.dynamic_update_slice(k_cache, jnp.concatenate(new_keys)[:, :, None, :], (0, 0, 0, 0))
        v_cache_out = lax.dynamic_update_slice(v_cache, jnp.concatenate(new_values)[:, :, None, :], (0, 0, 0, 0))
        return y.reshape(x.shape), k_cache_out, v_cache_out

    cache_spec = P("dp", None, "tp", None)
    return jax.shard_map(layer_shard, mesh=mesh, in_specs=(P("dp", None, None), P("dp"), P(None, "tp"), P(None, "tp"), P(None, "tp"), P("tp", None), P(None, "tp"), P(None, "tp"), P("tp", None), P(), P(), cache_spec, cache_spec), out_specs=(P("dp", None, None), cache_spec, cache_spec), check_vma=False)
```

```python
import functools

import jax
import jax.numpy as jnp
from jax import lax
from jax.experimental import pallas as pl
from jax.experimental.pallas import tpu as pltpu
from jax.sharding import PartitionSpec as P


EPS = 1e-5
ROPE_BASE = 10000.0
CHUNKS = (4, 6, 6, 5, 3)
PLACE_ROWS = 128
Q_BLOCK = 128
COL_TILE = 512


def norm_rows(src_ref, dst_ref, gain_ref, rows):
    def body(index, carry):
        parts = [pl.ds(pl.multiple_of(index * 48 + shift, 16), 16) for shift in (0, 16, 32)]
        inv_rms = []
        for part in parts:
            rows32 = src_ref[part, :].astype(jnp.float32)
            inv_rms.append(lax.rsqrt(jnp.mean(rows32 * rows32, axis=-1, keepdims=True) + EPS))
        for part, inv in zip(parts, inv_rms):
            dst_ref[part, :] = (src_ref[part, :].astype(jnp.float32) * inv * gain_ref[...].astype(jnp.float32)).astype(jnp.bfloat16)
        return carry

    lax.fori_loop(0, rows // 48, body, 0)


def attend_kernel(first, lens_ref, x_ref, wq_ref, wkv_ref, gain_ref, cos_ref, sin_ref, o_ref, k_ref, v_ref, normed_ref):
    seq_len = x_ref.shape[0]
    head_dim = cos_ref.shape[1]
    group_size = wq_ref.shape[1] // head_dim
    length = lens_ref[first + pl.program_id(0)]
    norm_rows(x_ref, normed_ref, gain_ref, seq_len)
    normed = normed_ref[...]
    kv_pre = jnp.dot(normed, wkv_ref[...], preferred_element_type=jnp.float32)
    q_pre = jnp.dot(normed, wq_ref[...], preferred_element_type=jnp.float32)
    cos_tab = cos_ref[...]
    sin_tab = sin_ref[...]
    even_lane = lax.broadcasted_iota(jnp.int32, (seq_len, head_dim), 1) % 2 == 0

    def rotate(vecs):
        swapped = jnp.where(even_lane, pltpu.roll(vecs, head_dim - 1, 1), pltpu.roll(vecs, 1, 1))
        return (vecs * cos_tab + swapped * sin_tab).astype(jnp.bfloat16)

    valid = lax.broadcasted_iota(jnp.int32, (seq_len, head_dim), 0) < length
    keys32 = jnp.where(valid, rotate(kv_pre[:, :head_dim]).astype(jnp.float32), 0.0)
    values32 = jnp.where(valid, kv_pre[:, head_dim:], 0.0)
    keys = keys32.astype(jnp.bfloat16)
    values = values32.astype(jnp.bfloat16)
    k_ref[...] = keys
    v_ref[...] = values
    queries = [rotate(q_pre[:, j * head_dim:(j + 1) * head_dim]) for j in range(group_size)]
    for block in range(seq_len // Q_BLOCK):
        lo, hi = block * Q_BLOCK, (block + 1) * Q_BLOCK
        t_pos = lo + lax.broadcasted_iota(jnp.int32, (Q_BLOCK, hi), 0)
        u_pos = lax.broadcasted_iota(jnp.int32, (Q_BLOCK, hi), 1)
        allowed = (u_pos <= t_pos) & (u_pos < length)
        for j in range(group_size):
            scores = lax.dot_general(queries[j][lo:hi], keys[:hi], (((1,), (1,)), ((), ())), preferred_element_type=jnp.float32) * head_dim ** -0.5
            scores = jnp.where(allowed, scores, -jnp.inf)
            expd = jnp.exp(scores - jnp.max(scores, axis=-1, keepdims=True))
            probs = (expd * (1.0 / jnp.sum(expd, axis=-1, keepdims=True))).astype(jnp.bfloat16)
            o_ref[lo:hi, j * head_dim:(j + 1) * head_dim] = jnp.dot(probs, values[:hi], preferred_element_type=jnp.float32).astype(jnp.bfloat16)


def attend(first, count, x, seq_lens, w_query, w_kv, gain, cos_tab, sin_tab):
    _, seq_len, width = x.shape
    q_cols = w_query.shape[1]
    head_dim = cos_tab.shape[1]
    whole = lambda *shape: pl.BlockSpec(shape, lambda b, lens: (0,) * len(shape))
    per_seq = lambda cols: pl.BlockSpec((None, seq_len, cols), lambda b, lens: (b, 0, 0))
    grid_spec = pltpu.PrefetchScalarGridSpec(
        num_scalar_prefetch=1,
        grid=(count,),
        in_specs=[
            pl.BlockSpec((None, seq_len, width), lambda b, lens: (first + b, 0, 0)),
            whole(width, q_cols),
            whole(width, 2 * head_dim),
            whole(1, width),
            whole(seq_len, head_dim),
            whole(seq_len, head_dim),
        ],
        out_specs=[per_seq(q_cols), per_seq(head_dim), per_seq(head_dim)],
        scratch_shapes=[pltpu.VMEM((seq_len, width), jnp.bfloat16)],
    )
    return pl.pallas_call(
        functools.partial(attend_kernel, first),
        grid_spec=grid_spec,
        out_shape=[jax.ShapeDtypeStruct((count, seq_len, cols), jnp.bfloat16) for cols in (q_cols, head_dim, head_dim)],
        compiler_params=pltpu.CompilerParams(vmem_limit_bytes=56 * 1024 * 1024),
        cost_estimate=pl.CostEstimate(flops=2 * count * seq_len * width * (q_cols + 2 * head_dim), bytes_accessed=2 * count * seq_len * (width + q_cols), transcendentals=0),
        name="attend",
    )(seq_lens, x, w_query, w_kv, gain, cos_tab, sin_tab)


def project_kernel(o_ref, w_ref, x_ref, gain_ref, h_ref, n_ref):
    groups, rows, depth = o_ref.shape
    tile = w_ref.shape[1]
    columns = pl.ds(pl.multiple_of(pl.program_id(0) * tile, tile), tile)
    total = jnp.zeros((rows, tile), jnp.float32)
    for index in range(groups):
        partial = jnp.dot(o_ref[index], w_ref[index * depth:(index + 1) * depth, :], preferred_element_type=jnp.float32)
        total = total + partial.astype(jnp.bfloat16).astype(jnp.float32)
    h_ref[:, columns] = (x_ref[...].astype(jnp.float32) + total).astype(jnp.bfloat16)

    @pl.when(pl.program_id(0) == pl.num_programs(0) - 1)
    def _():
        norm_rows(h_ref, n_ref, gain_ref, rows)


def project(o_all, w_out_all, x_rows, gain):
    groups, rows, depth = o_all.shape
    width = w_out_all.shape[1]
    out = jax.ShapeDtypeStruct((rows, width), jnp.bfloat16)
    return pl.pallas_call(
        project_kernel,
        grid=(width // COL_TILE,),
        in_specs=[
            pl.BlockSpec((groups, rows, depth), lambda j: (0, 0, 0)),
            pl.BlockSpec((groups * depth, COL_TILE), lambda j: (0, j)),
            pl.BlockSpec((rows, COL_TILE), lambda j: (0, j)),
            pl.BlockSpec((1, width), lambda j: (0, 0)),
        ],
        out_specs=[pl.BlockSpec((rows, width), lambda j: (0, 0))] * 2,
        out_shape=[out, out],
        compiler_params=pltpu.CompilerParams(vmem_limit_bytes=48 * 1024 * 1024),
        cost_estimate=pl.CostEstimate(flops=2 * rows * groups * depth * width, bytes_accessed=2 * (groups * depth * width + 4 * rows * width), transcendentals=0),
        name="project",
    )(o_all, w_out_all, x_rows, gain)


def place_kernel(block_ref, *refs):
    refs[-1][...] = block_ref[...]


def place(y, block, start, total_rows):
    rows, width = block.shape
    operands = [block] if y is None else [block, y]
    return pl.pallas_call(
        place_kernel,
        grid=(rows // PLACE_ROWS,),
        in_specs=[pl.BlockSpec((PLACE_ROWS, width), lambda i: (i, 0)), pl.BlockSpec(memory_space=pl.ANY)][:len(operands)],
        out_specs=pl.BlockSpec((PLACE_ROWS, width), lambda i: (start // PLACE_ROWS + i, 0)),
        out_shape=jax.ShapeDtypeStruct((total_rows, width), jnp.bfloat16),
        input_output_aliases={} if y is None else {1: 0},
        compiler_params=pltpu.CompilerParams(vmem_limit_bytes=60 * 1024 * 1024),
        cost_estimate=pl.CostEstimate(flops=rows * width, bytes_accessed=4 * rows * width, transcendentals=0),
        name="place",
    )(*operands)


def solution(mesh):
    tp_size = mesh.shape["tp"]
    last = len(CHUNKS) - 1

    def swap(value, bit):
        return lax.ppermute(value, "tp", [(index, index ^ bit) for index in range(tp_size)])

    def sum_partials(partial, resid_rows):
        rows, width = resid_rows.shape
        half = rows // 2
        me = lax.axis_index("tp")
        core, chip = me % 2, me // 2
        theirs = swap(partial, 1)

        def both(step, lo):
            start = (2 * (chip ^ step) + core) * rows + lo
            pick = lambda value: lax.dynamic_slice(value, (start, 0), (half, width)).astype(jnp.float32)
            return pick(partial) + pick(theirs)

        x_far, y_far = swap(both(3, 0), 2), swap(both(3, half), 4)
        x_near, y_near = swap(both(1, 0), 2), swap(both(2, half), 4)
        x_late = swap(both(1, half) + y_far, 2)
        y_late = swap(both(2, 0) + x_far, 4)
        upper = resid_rows[:half].astype(jnp.float32) + (both(0, 0) + x_near + y_late)
        lower = resid_rows[half:].astype(jnp.float32) + (both(0, half) + x_late + y_near)
        return jnp.concatenate([upper.astype(jnp.bfloat16), lower.astype(jnp.bfloat16)], axis=0)

    def layer_shard(x, seq_lens, w_query, w_key, w_value, w_out, w_gate, w_up, w_down, attn_gain, mlp_gain, k_cache, v_cache):
        batch_size, seq_len, width = x.shape
        head_dim = k_cache.shape[3]
        tp_index = lax.axis_index("tp")
        w_out_all = lax.all_gather(w_out, "tp", axis=0, tiled=True)
        w_kv = jnp.concatenate([w_key, w_value], axis=1)
        inv_freq = ROPE_BASE ** (-jnp.arange(0, head_dim, 2).astype(jnp.float32) / head_dim)
        angles = jnp.repeat(jnp.arange(seq_len).astype(jnp.float32)[:, None] * inv_freq[None, :], 2, axis=1)
        sign = jnp.where(jnp.arange(head_dim) % 2 == 0, -1.0, 1.0)
        cos_tab = jnp.cos(angles)
        sin_tab = jnp.sin(angles) * sign
        x_flat = x.reshape(batch_size * seq_len, width)
        y = None
        gathered = []

        def settle(y, block, index):
            return place(y, block, sum(CHUNKS[:index]) * seq_len, batch_size * seq_len)

        starts = [sum(CHUNKS[:index]) for index in range(len(CHUNKS))]
        attended, received = [], []
        for first, count in zip(starts, CHUNKS):
            attended.append(attend(first, count, x, seq_lens, w_query, w_kv, attn_gain[None], cos_tab, sin_tab))
            received.append(lax.all_to_all(attended[-1][0].reshape(tp_size, count * seq_len // tp_size, -1), "tp", 0, 0, tiled=True))
        new_keys = [keys for _, keys, _ in attended]
        new_values = [values for _, _, values in attended]
        w_out_all, early_keys = lax.optimization_barrier((w_out_all, new_keys[:last]))
        new_keys = early_keys + new_keys[last:]
        for index, (first, count) in enumerate(zip(starts, CHUNKS)):
            start_row = first * seq_len
            rows = count * seq_len // tp_size
            x_rows = lax.dynamic_slice_in_dim(x_flat, start_row + tp_index * rows, rows, axis=0)
            hidden, normed = project(received[index], w_out_all, x_rows, mlp_gain[None])
            normed_all = lax.all_gather(normed, "tp", axis=0, tiled=True)
            gate_pre = jnp.dot(normed_all, w_gate, preferred_element_type=jnp.float32)
            up_pre = jnp.dot(normed_all, w_up, preferred_element_type=jnp.float32)
            gated = (jax.nn.silu(gate_pre) * up_pre).astype(jnp.bfloat16)
            mlp_part = jnp.dot(gated, w_down, preferred_element_type=jnp.float32).astype(jnp.bfloat16)
            if index >= 2:
                y = settle(y, gathered[index - 2], index - 2)
            out_rows = sum_partials(mlp_part, hidden)
            gathered.append(lax.all_gather(out_rows, "tp", axis=0, tiled=True))
        for index in (last - 1, last):
            y = settle(y, gathered[index], index)
        k_cache_out = lax.dynamic_update_slice(k_cache, jnp.concatenate(new_keys)[:, :, None, :], (0, 0, 0, 0))
        v_cache_out = lax.dynamic_update_slice(v_cache, jnp.concatenate(new_values)[:, :, None, :], (0, 0, 0, 0))
        return y.reshape(x.shape), k_cache_out, v_cache_out

    cache_spec = P("dp", None, "tp", None)
    return jax.shard_map(layer_shard, mesh=mesh, in_specs=(P("dp", None, None), P("dp"), P(None, "tp"), P(None, "tp"), P(None, "tp"), P("tp", None), P(None, "tp"), P(None, "tp"), P("tp", None), P(), P(), cache_spec, cache_spec), out_specs=(P("dp", None, None), cache_spec, cache_spec), check_vma=False)
```
